128 devices in a mesh: inter: 2 (over y_hi), intra: 64 (over x, y_lo, z, core).
Axes of the slice: x: 4, y: 4 (y_hi: 2, y_lo: 2; y = y_hi * 2 + y_lo), z: 4, core: 2. Of those that a mesh axis runs over, the one named last changes fastest.
Arguments:
- activations: bfloat16 [262144, 4096], P(('inter', 'intra')), may hold values from -6 to 6
- key_cotangent: bfloat16 [262144, 512], P(('inter', 'intra')), may hold values from -0.046875 to 0.046875
- value_cotangent: bfloat16 [262144, 512], P(('inter', 'intra')), may hold values from -0.046875 to 0.046875
Outputs:
- grad_key: float32 [4096, 512], P('intra')
- grad_value: float32 [4096, 512], P('intra')
The draws below stay inside these ranges and needn't reach their ends.
All inputs are finite; a program needn't handle non-finite values.
Results may differ from the reference program's by a relative error of at most 0.0029.
Values sent between devices are 32-bit elements; how exact they have to be, the bound alone decides.
A program may use at most 128 MiB of HBM per device.

```python
import jax
import jax.numpy as jnp
from jax import lax

D = 4096
TOK_DEV = 2048
KV = 512
TOKENS = 262144
N_INTER = 2
N_INTRA = 64


def levels(key, dims, split, low, largest):
    level, own = 1.0, jax.random.fold_in(key, 6)
    for dim, blocks in split:
        heights = jnp.exp(jax.random.uniform(jax.random.fold_in(own, dim), (blocks,), jnp.float32, low / len(split), largest / len(split)))
        level = level * jnp.repeat(heights, dims[dim] // blocks).reshape([-1 if axis == dim else 1 for axis in range(len(dims))])
    return level


def centred(stream_key, shape, spread, limit, cuts=(), kind=jnp.bfloat16):
    values = spread * jax.random.normal(stream_key, shape, jnp.float32)
    if cuts:
        values = values * levels(stream_key, shape, cuts, -0.22, 0.18)
    return jnp.clip(values, -limit, limit).astype(kind)


def setup_inputs(seed: int = 0) -> dict:
    arg_keys = jax.random.split(jax.random.key(seed), 4)
    activations = centred(arg_keys[0], (TOKENS, D), 1.0, 6.0, ((0, 128),))
    key_cotangent = centred(arg_keys[1], (TOKENS, KV), 0.003, 0.046875, ((0, 128),))
    value_cotangent = centred(arg_keys[2], (TOKENS, KV), 0.003, 0.046875, ((0, 128),))
    return dict(activations=activations, key_cotangent=key_cotangent, value_cotangent=value_cotangent)


def accumulate(total, inputs):
    rows, cotangent = inputs
    device_term = jnp.dot(rows.T, cotangent, preferred_element_type=jnp.float32)
    rounded = lax.optimization_barrier(device_term.astype(jnp.bfloat16))
    return total + rounded.astype(jnp.float32), None


def reference(activations, key_cotangent, value_cotangent):
    devices = N_INTER * N_INTRA
    stacked_rows = activations.reshape(devices, TOK_DEV, D)
    cotangent = jnp.concatenate((key_cotangent, value_cotangent), axis=1).reshape(devices, TOK_DEV, 2 * KV)
    total = lax.scan(accumulate, jnp.zeros((D, 2 * KV), jnp.float32), (stacked_rows, cotangent))[0]
    return total[:, :KV], total[:, KV:]
```

```python
import functools

import jax
import jax.numpy as jnp
from jax import lax
from jax.experimental import pallas as pl
from jax.experimental.pallas import tpu as pltpu
from jax.sharding import Mesh
from jax.sharding import PartitionSpec as P

MESH = pl.DeviceIdType.MESH
F32 = jnp.float32
AXES = ("inter", "x", "ylo", "z", "core")
INTRA = ("x", "ylo", "z", "core")

ORDER = {"x": (2, 1, 3, 0), "y": (1, 2, 3, 0), "z": (1, 2, 3, 0)}
SIZES = (48, 40, 40, 40, 48, 40)
KEEP = 3
LAG = 4


def flip(r, k):
    if k == 0:
        return r
    if k == 1:
        return r + 1 - 2 * (r % 2)
    if k == 2:
        return (r + 2) % 4
    return 3 - r


def colours():
    result, off = [], 0
    index = 0
    for order in ("xyz", "yzx", "zxy"):
        for p1, p2 in ((1, 3), (3, 1)):
            result.append((index, order, p1, p2, pl.ds(off, SIZES[index])))
            off += SIZES[index]
            index += 1
    return result


def slot(axis, k):
    return ORDER[axis].index(k)


def pair_start(p1):
    return 0 if p1 == 1 else 1


def pair_item(p1, keep):
    first_is_keep = p1 == 1
    return 0 if first_is_keep == keep else 1


def kernel(
    a_hbm, k_hbm, v_hbm, out_k, out_v,
    abuf, cst, ct, acc, dsend, drecv, r1, r2, r3, r4, r5, r6, fin, obuf,
    a_sem, c_sem, ds_sem, dr_sem, s1s, s1r, s2s, s2r, s3s, s3r, s4s, s4r, s5s, s5r, s6s, s6r, fs_sem, fr_sem,
):
    tok = a_hbm.shape[0]
    x, z = lax.axis_index("x"), lax.axis_index("z")
    yhi, ylo = lax.axis_index("inter"), lax.axis_index("ylo")
    core = lax.axis_index("core")
    y = 2 * yhi + ylo
    cols = colours()

    def peer(axis, k):
        if axis == "x":
            return {"x": flip(x, k)}
        if axis == "z":
            return {"z": flip(z, k)}
        to = flip(y, k)
        return {"inter": to // 2, "ylo": to % 2}

    other_core = {"core": 1 - core}
    far = {"inter": 1 - yhi}
    far_other = {"inter": 1 - yhi, "core": 1 - core}

    barrier = pltpu.get_barrier_semaphore()
    peers = [other_core, far, far_other] + [peer(axis, k) for axis in "xyz" for k in (1, 3)]
    for device in peers:
        pl.semaphore_signal(barrier, inc=1, device_id=device, device_id_type=MESH)

    def c_copy(which, hrel):
        src = (k_hbm, v_hbm)[which]
        rel = core if which == 0 else 1 - core
        half = (yhi + hrel) % 2
        return pltpu.make_async_copy(
            src.at[:, pl.ds(pl.multiple_of(half * 256, 256), 256)], cst.at[rel, hrel], c_sem.at[which, hrel]
        )

    for which in (0, 1):
        for hrel in (0, 1):
            c_copy(which, hrel).start()

    def a_copy(u, lrel, column):
        return pltpu.make_async_copy(
            a_hbm.at[:, pl.ds(column, 128)], abuf.at[u, :, pl.ds(lrel * 128, 128)], a_sem.at[u, lrel]
        )

    for sx in range(4):
        for sz in range(4):
            for lrel in (0, 1):
                tx, tz = flip(x, ORDER["x"][sx]), flip(z, ORDER["z"][sz])
                tl = (ylo + lrel) % 2
                column = pl.multiple_of(((tx * 2 + tl) * 4 + tz) * 128, 128)
                a_copy(sx * 4 + sz, lrel, column).start()

    for which in (0, 1):
        for hrel in (0, 1):
            c_copy(which, hrel).wait()
    for rel in (1, 0):
        for hrel in (0, 1):
            ct[rel, pl.ds(hrel * 256, 256), :] = cst[rel, hrel].T

    pl.semaphore_wait(barrier, len(peers))

    def remote(src, dst, send, recv, device):
        return pltpu.make_async_remote_copy(
            src_ref=src, dst_ref=dst, send_sem=send, recv_sem=recv, device_id=device, device_id_type=MESH
        )

    def d2d(v):
        return remote(dsend.at[v], drecv.at[v], ds_sem.at[v], dr_sem.at[v], other_core)

    def send1(c, v, sx, sz, i, j):
        index, order, p1, p2, rows = c
        axis = order[0]
        if axis == "y":
            src = acc.at[sx, sz, pl.ds(pair_start(p1), 2), rows]
            return remote(src, r1.at[pl.ds(v * 2, 2), rows], s1s.at[index, v], s1r.at[index, v], peer(axis, p1))
        n = i * 4 + j
        return remote(
            acc.at[sx, sz, :, rows], r1.at[pl.ds(n * 4, 4), rows], s1s.at[index, n], s1r.at[index, n], peer(axis, p1)
        )

    def send2(c, sx, sz, n):
        index, order, p1, p2, rows = c
        axis = order[0]
        if axis == "y":
            src = acc.at[sx, sz, slot("y", p2), rows]
            return remote(src, r2.at[n, rows], s2s.at[index, n], s2r.at[index, n], peer(axis, p2))
        return remote(
            acc.at[sx, sz, :, rows], r2.at[pl.ds(n * 4, 4), rows], s2s.at[index, n], s2r.at[index, n], peer(axis, p2)
        )

    def process(v):
        sx, sz = v // 4, v % 4
        d2d(v).wait_recv()
        acc[sx, sz] = acc[sx, sz] + drecv[v]
        for c in cols:
            index, order, p1, p2, rows = c
            if order[0] == "y":
                send1(c, v, sx, sz, 0, 0).start()
            else:
                axis = order[0]
                mine, rest = (sx, sz) if axis == "x" else (sz, sx)
                for i, k in ((0, 2), (1, p1)):

                    @pl.when(mine == slot(axis, k))
                    def _(c=c, i=i, rest=rest):
                        send1(c, v, sx, sz, i, rest).start()

    def process2(v):
        sx, sz = v // 4, v % 4
        for c in cols:
            index, order, p1, p2, rows = c
            axis = order[0]
            if axis == "y":
                send1(c, v, sx, sz, 0, 0).wait_recv()
                on = slot("y", p2)
                acc[sx, sz, on, rows] = acc[sx, sz, on, rows] + r1[v * 2 + pair_item(p1, False), rows]
                acc[sx, sz, KEEP, rows] = acc[sx, sz, KEEP, rows] + r1[v * 2 + pair_item(p1, True), rows]
                send2(c, sx, sz, v).start()
            elif axis == "x":

                @pl.when(sx == slot("x", p2))
                def _(c=c, index=index, rows=rows):
                    send1(c, v, sx, sz, 0, sz).wait_recv()
                    acc[sx, sz, :, rows] = acc[sx, sz, :, rows] + r1[pl.ds(sz * 4, 4), rows]
                    send2(c, sx, sz, sz).start()
            else:

                @pl.when(sz == 3)
                def _(c=c, p2=p2, rows=rows):
                    on = slot("z", p2)
                    send1(c, v, sx, on, 0, sx).wait_recv()
                    acc[sx, on, :, rows] = acc[sx, on, :, rows] + r1[pl.ds(sx * 4, 4), rows]
                    send2(c, sx, on, sx).start()

    def step(u, carry):
        @pl.when(u < 16)
        def _():
            sx, sz = u // 4, u % 4
            a_copy(u, 0, 0).wait()
            a_copy(u, 1, 0).wait()
            for rel in (1, 0):
                product = jnp.dot(ct[rel], abuf[u], preferred_element_type=F32)
                for hrel in (0, 1):
                    for lrel in (0, 1):
                        block = product[hrel * 256 : hrel * 256 + 256, lrel * 128 : lrel * 128 + 128]
                        target = slot("y", 2 * hrel + lrel)
                        if rel == 1:
                            dsend[u, target] = block
                        else:
                            acc[sx, sz, target] = block
                if rel == 1:
                    d2d(u).start()

        @pl.when((u >= 1) & (u <= 16))
        def _():
            process(u - 1)

        @pl.when(u >= LAG)
        def _():
            process2(u - LAG)

        return carry

    lax.fori_loop(0, 16 + LAG, step, 0)

    xs, ys, zs = cols[0:2], cols[2:4], cols[4:6]

    def x_send3(c, sz):
        index, _, p1, _, rows = c
        return remote(
            acc.at[3, sz, pl.ds(pair_start(p1), 2), rows], r3.at[pl.ds(sz * 2, 2), rows],
            s3s.at[index, sz], s3r.at[index, sz], peer("y", p1),
        )

    def y_send3(c, sx):
        index, _, p1, _, rows = c
        return remote(
            acc.at[sx, pl.ds(pair_start(p1), 2), KEEP, rows], r3.at[pl.ds(sx * 2, 2), rows],
            s3s.at[index, sx], s3r.at[index, sx], peer("z", p1),
        )

    def z_send3(c, i):
        index, _, p1, _, rows = c
        sx = slot("x", (2, p1)[i])
        return remote(
            acc.at[sx, KEEP, :, rows], r3.at[pl.ds(i * 4, 4), rows],
            s3s.at[index, i], s3r.at[index, i], peer("x", p1),
        )

    for sz in range(4):
        for c in xs:
            rows = c[4]
            send1(c, 0, 0, 0, 1, sz).wait_recv()
            send2(c, 0, 0, sz).wait_recv()
            acc[3, sz, :, rows] = acc[3, sz, :, rows] + (r1[pl.ds(16 + sz * 4, 4), rows] + r2[pl.ds(sz * 4, 4), rows])
            x_send3(c, sz).start()

    for sx in range(4):
        for c in zs:
            _, _, p1, _, rows = c
            send1(c, 0, 0, 0, 1, sx).wait_recv()
            send2(c, 0, 0, sx).wait_recv()
            acc[sx, 3, :, rows] = acc[sx, 3, :, rows] + (r1[pl.ds(16 + sx * 4, 4), rows] + r2[pl.ds(sx * 4, 4), rows])
            for i in (0, 1):
                if sx == slot("x", (2, p1)[i]):
                    z_send3(c, i).start()
        for c in ys:
            rows = c[4]
            for sz in range(4):
                send2(c, 0, 0, sx * 4 + sz).wait_recv()
            acc[sx, :, KEEP, rows] = acc[sx, :, KEEP, rows] + r2[pl.ds(sx * 4, 4), rows]
            y_send3(c, sx).start()

    def x_send4(c):
        index, _, _, p2, rows = c
        return remote(acc.at[3, :, slot("y", p2), rows], r4.at[:, rows], s4s.at[index], s4r.at[index], peer("y", p2))

    def y_send4(c):
        index, _, _, p2, rows = c
        return remote(acc.at[:, slot("z", p2), KEEP, rows], r4.at[:, rows], s4s.at[index], s4r.at[index], peer("z", p2))

    def z_send4(c):
        index, _, _, p2, rows = c
        return remote(acc.at[slot("x", p2), KEEP, :, rows], r4.at[:, rows], s4s.at[index], s4r.at[index], peer("x", p2))

    for c in xs:
        _, _, p1, p2, rows = c
        on = slot("y", p2)
        for sz in range(4):
            x_send3(c, sz).wait_recv()
            acc[3, sz, on, rows] = acc[3, sz, on, rows] + r3[sz * 2 + pair_item(p1, False), rows]
            acc[3, sz, KEEP, rows] = acc[3, sz, KEEP, rows] + r3[sz * 2 + pair_item(p1, True), rows]
        x_send4(c).start()
    for c in zs:
        _, _, p1, p2, rows = c
        on = slot("x", p2)
        z_send3(c, 0).wait_recv()
        acc[on, KEEP, :, rows] = acc[on, KEEP, :, rows] + r3[pl.ds(0, 4), rows]
        z_send4(c).start()
    for c in ys:
        _, _, p1, p2, rows = c
        on = slot("z", p2)
        for sx in range(4):
            y_send3(c, sx).wait_recv()
            acc[sx, on, KEEP, rows] = acc[sx, on, KEEP, rows] + r3[sx * 2 + pair_item(p1, False), rows]
            acc[sx, 3, KEEP, rows] = acc[sx, 3, KEEP, rows] + r3[sx * 2 + pair_item(p1, True), rows]
        y_send4(c).start()

    def x_send5(c):
        index, _, p1, _, rows = c
        return remote(
            acc.at[3, pl.ds(pair_start(p1), 2), KEEP, rows], r5.at[:, rows], s5s.at[index, 0], s5r.at[index, 0], peer("z", p1)
        )

    def z_send5(c):
        index, _, p1, _, rows = c
        return remote(
            acc.at[3, KEEP, pl.ds(pair_start(p1), 2), rows], r5.at[:, rows], s5s.at[index, 0], s5r.at[index, 0], peer("y", p1)
        )

    def y_send5(c, i):
        index, _, p1, _, rows = c
        return remote(
            acc.at[slot("x", (2, p1)[i]), KEEP, KEEP, rows], r5.at[i, rows], s5s.at[index, i], s5r.at[index, i], peer("x", p1)
        )

    for c in xs:
        rows = c[4]
        x_send4(c).wait_recv()
        acc[3, :, KEEP, rows] = acc[3, :, KEEP, rows] + r4[:, rows]
        x_send5(c).start()
    for c in zs:
        _, _, p1, _, rows = c
        z_send3(c, 1).wait_recv()
        z_send4(c).wait_recv()
        acc[3, KEEP, :, rows] = acc[3, KEEP, :, rows] + (r3[pl.ds(4, 4), rows] + r4[:, rows])
        z_send5(c).start()
    for c in ys:
        rows = c[4]
        y_send4(c).wait_recv()
        acc[:, 3, KEEP, rows] = acc[:, 3, KEEP, rows] + r4[:, rows]
        for i in (0, 1):
            y_send5(c, i).start()

    def last(c, axis):
        index, _, _, p2, rows = c
        on = slot(axis, p2)
        src = {"x": acc.at[on, KEEP, KEEP, rows], "y": acc.at[3, KEEP, on, rows], "z": acc.at[3, on, KEEP, rows]}[axis]
        return remote(src, r6.at[rows], s6s.at[index], s6r.at[index], peer(axis, p2))

    for group, axis in ((xs, "z"), (zs, "y"), (ys, "x")):
        for c in group:
            _, _, p1, p2, rows = c
            on = slot(axis, p2)
            if axis == "x":
                y_send5(c, 0).wait_recv()
                y_send5(c, 1).wait_recv()
                onward, kept = r5[0, rows], r5[1, rows]
                acc[on, KEEP, KEEP, rows] = acc[on, KEEP, KEEP, rows] + onward
            else:
                (x_send5 if axis == "z" else z_send5)(c).wait_recv()
                onward, kept = r5[pair_item(p1, False), rows], r5[pair_item(p1, True), rows]
                if axis == "z":
                    acc[3, on, KEEP, rows] = acc[3, on, KEEP, rows] + onward
                else:
                    acc[3, KEEP, on, rows] = acc[3, KEEP, on, rows] + onward
            last(c, axis).start()
            acc[3, KEEP, KEEP, rows] = acc[3, KEEP, KEEP, rows] + kept

    for group, axis in ((xs, "z"), (zs, "y"), (ys, "x")):
        for c in group:
            last(c, axis).wait_recv()

    fin[...] = (acc[3, KEEP, KEEP] + r6[...]).T
    place = pl.ds(pl.multiple_of(yhi * 256, 256), 256)

    def spread(n, to_core, device):
        return remote(
            fin.at[pl.ds(to_core * 64, 64)], obuf.at[core, :, place], fs_sem.at[n], fr_sem.at[n], device
        )

    sends = (
        spread(0, core, far), spread(1, 1 - core, far_other), spread(2, 1 - core, other_core),
    )
    for copy in sends:
        copy.start()
    obuf[core, :, place] = fin[pl.ds(core * 64, 64)]
    for copy in sends:
        copy.wait_recv()
    out_k[...] = obuf[0]
    out_v[...] = obuf[1]

    def units(v, carry):
        d2d(v).wait_send()
        for c in ys:
            send1(c, v, v // 4, v % 4, 0, 0).wait_send()
            send2(c, v // 4, v % 4, v).wait_send()
        return carry

    lax.fori_loop(0, 16, units, 0)

    def groups(n, carry):
        for c in xs + zs:
            send1(c, 0, 0, 0, 0, n).wait_send()
            send1(c, 0, 0, 0, 1, n).wait_send()
            send2(c, 0, 0, n).wait_send()
        for c in xs:
            x_send3(c, n).wait_send()
        for c in ys:
            y_send3(c, n).wait_send()
        return carry

    lax.fori_loop(0, 4, groups, 0)
    for c in zs:
        z_send3(c, 0).wait_send()
        z_send3(c, 1).wait_send()
        z_send4(c).wait_send()
        z_send5(c).wait_send()
        last(c, "y").wait_send()
    for c in xs:
        x_send4(c).wait_send()
        x_send5(c).wait_send()
        last(c, "z").wait_send()
    for c in ys:
        y_send4(c).wait_send()
        y_send5(c, 0).wait_send()
        y_send5(c, 1).wait_send()
        last(c, "x").wait_send()
    for copy in sends:
        copy.wait_send()


def local(activations, key_cotangent, value_cotangent):
    tok, width = activations.shape
    half = key_cotangent.shape[1]
    rows = width // 64
    dma = pltpu.SemaphoreType.DMA
    return pl.pallas_call(
        kernel,
        out_shape=(jax.ShapeDtypeStruct((rows, half), F32), jax.ShapeDtypeStruct((rows, half), F32)),
        in_specs=[pl.BlockSpec(memory_space=pl.ANY)] * 3,
        out_specs=(pl.BlockSpec(memory_space=pltpu.VMEM), pl.BlockSpec(memory_space=pltpu.VMEM)),
        scratch_shapes=[
            pltpu.VMEM((16, tok, 256), jnp.bfloat16),
            pltpu.VMEM((2, 2, tok, 256), jnp.bfloat16),
            pltpu.VMEM((2, 512, tok), jnp.bfloat16),
            pltpu.VMEM((4, 4, 4, 256, 128), F32),
            pltpu.VMEM((16, 4, 256, 128), F32),
            pltpu.VMEM((16, 4, 256, 128), F32),
            pltpu.VMEM((32, 256, 128), F32),
            pltpu.VMEM((16, 256, 128), F32),
            pltpu.VMEM((8, 256, 128), F32),
            pltpu.VMEM((4, 256, 128), F32),
            pltpu.VMEM((2, 256, 128), F32),
            pltpu.VMEM((256, 128), F32),
            pltpu.VMEM((128, 256), F32),
            pltpu.VMEM((2, rows, half), F32),
            dma((16, 2)), dma((2, 2)), dma((16,)), dma((16,)),
            dma((6, 16)), dma((6, 16)), dma((6, 16)), dma((6, 16)),
            dma((6, 4)), dma((6, 4)), dma((6,)), dma((6,)),
            dma((6, 2)), dma((6, 2)), dma((6,)), dma((6,)),
            dma((3,)), dma((3,)),
        ],
        compiler_params=pltpu.CompilerParams(
            collective_id=0, has_side_effects=True, vmem_limit_bytes=67_043_328
        ),
        name="weight_gradients",
    )(activations, key_cotangent, value_cotangent)


def solution(mesh):
    finer = Mesh(mesh.devices.reshape(mesh.shape["inter"], 4, 2, 4, 2), AXES)
    spec = P(AXES, None)
    out = P(INTRA, None)
    return jax.shard_map(local, mesh=finer, in_specs=(spec, spec, spec), out_specs=(out, out), check_vma=False)
```

```python
import functools

import jax
import jax.numpy as jnp
from jax import lax
from jax.experimental import pallas as pl
from jax.experimental.pallas import tpu as pltpu
from jax.sharding import Mesh
from jax.sharding import PartitionSpec as P

MESH = pl.DeviceIdType.MESH
F32 = jnp.float32
AXES = ("inter", "x", "ylo", "z", "core")
INTRA = ("x", "ylo", "z", "core")

ORDER = {"x": (2, 1, 3, 0), "y": (1, 2, 3, 0), "z": (1, 2, 3, 0)}
SIZES = (48, 40, 40, 40, 48, 40)
KEEP = 3
LAG1 = 1
LAG2 = 3


def flip(r, k):
    if k == 0:
        return r
    if k == 1:
        return r + 1 - 2 * (r % 2)
    if k == 2:
        return (r + 2) % 4
    return 3 - r


def colours():
    result, off = [], 0
    index = 0
    for order in ("xyz", "yzx", "zxy"):
        for p1, p2 in ((1, 3), (3, 1)):
            result.append((index, order, p1, p2, pl.ds(off, SIZES[index])))
            off += SIZES[index]
            index += 1
    return result


def slot(axis, k):
    return ORDER[axis].index(k)


def pair_start(p1):
    return 0 if p1 == 1 else 1


def pair_item(p1, keep):
    first_is_keep = p1 == 1
    return 0 if first_is_keep == keep else 1


def kernel(
    a_hbm, k_hbm, v_hbm, out_k, out_v,
    abuf, cst, ct, acc, dsend, drecv, r1, r2, r3, r4, r5, r6, afar, fin, obuf,
    a_sem, c_sem, ds_sem, dr_sem, s1s, s1r, s2s, s2r, s3s, s3r, s4s, s4r, s5s, s5r, s6s, s6r, fs_sem, fr_sem, es_sem, er_sem,
):
    x, z = lax.axis_index("x"), lax.axis_index("z")
    yhi, ylo = lax.axis_index("inter"), lax.axis_index("ylo")
    core = lax.axis_index("core")
    y = 2 * yhi + ylo
    cols = colours()
    xs, ys, zs = cols[0:2], cols[2:4], cols[4:6]

    def peer(axis, k):
        if axis == "x":
            return {"x": flip(x, k)}
        if axis == "z":
            return {"z": flip(z, k)}
        to = flip(y, k)
        return {"inter": to // 2, "ylo": to % 2}

    other_core = {"core": 1 - core}
    far = {"inter": 1 - yhi}

    barrier = pltpu.get_barrier_semaphore()
    peers = [other_core, far] + [peer(axis, k) for axis in "xyz" for k in (1, 3)]
    for device in peers:
        pl.semaphore_signal(barrier, inc=1, device_id=device, device_id_type=MESH)

    def c_copy(which, hrel):
        src = (k_hbm, v_hbm)[which]
        rel = core if which == 0 else 1 - core
        half = (yhi + hrel) % 2
        return pltpu.make_async_copy(
            src.at[:, pl.ds(pl.multiple_of(half * 256, 256), 256)], cst.at[rel, hrel], c_sem.at[which, hrel]
        )

    def a_start(t):
        for n in range(4):
            tx, tz = flip(x, ORDER["x"][t // 2]), flip(z, ORDER["z"][t % 2 * 2 + n // 2])
            column = pl.multiple_of(((tx * 2 + (ylo + n) % 2) * 4 + tz) * 128, 128)
            pltpu.make_async_copy(
                a_hbm.at[:, pl.ds(column, 128)], abuf.at[t, :, pl.ds(n * 128, 128)], a_sem.at[t]
            ).start()

    with jax.named_scope("cwait"):
        for which in (0, 1):
            for hrel in (0, 1):
                c_copy(which, hrel).start()
        a_start(0)
        for which in (0, 1):
            for hrel in (0, 1):
                c_copy(which, hrel).wait()
    for t in range(1, 8):
        a_start(t)

    def transpose(rel):
        for hrel in (0, 1):
            ct[rel, pl.ds(hrel * 256, 256), :] = cst[rel, hrel].T

    with jax.named_scope("ctrans"):
        transpose(1)

    pl.semaphore_wait(barrier, len(peers))

    def remote(src, dst, send, recv, device):
        return pltpu.make_async_remote_copy(
            src_ref=src, dst_ref=dst, send_sem=send, recv_sem=recv, device_id=device, device_id_type=MESH
        )

    def d2d(t):
        return remote(dsend.at[t], drecv.at[t], ds_sem, dr_sem.at[t], other_core)

    def x_send1(c, sx, sp, i):
        index, _, p1, _, rows = c
        return remote(
            acc.at[sx, pl.ds(2 * sp, 2), :, rows], r1.at[pl.ds(i * 4 + 2 * sp, 2), :, rows],
            s1s, s1r.at[index, i * 2 + sp], peer("x", p1),
        )

    def z_send1(c, sx, sz, i):
        index, _, p1, _, rows = c
        return remote(
            acc.at[sx, sz, :, rows], r1.at[i * 4 + sx, :, rows], s1s, s1r.at[index, i * 4 + sx], peer("z", p1)
        )

    def y_send1(c, t, sx, sp, n):
        index, _, p1, _, rows = c
        return remote(
            acc.at[sx, 2 * sp + n, pl.ds(pair_start(p1), 2), rows], r1.at[t, pl.ds(n * 2, 2), rows],
            s1s, s1r.at[index, t], peer("y", p1),
        )

    def y_wait1(c, t):
        index, _, p1, _, rows = c
        remote(r1.at[t, :, rows], r1.at[t, :, rows], s1s, s1r.at[index, t], peer("y", p1)).wait_recv()

    def x_send2(c, sx, sp):
        index, _, _, p2, rows = c
        return remote(
            acc.at[sx, pl.ds(2 * sp, 2), :, rows], r2.at[pl.ds(2 * sp, 2), :, rows], s2s, s2r.at[index, sp], peer("x", p2)
        )

    def z_send2(c, sx, sz):
        index, _, _, p2, rows = c
        return remote(acc.at[sx, sz, :, rows], r2.at[sx, :, rows], s2s, s2r.at[index, sx], peer("z", p2))

    def y_send2(c, t, sx, sp):
        index, _, _, p2, rows = c
        return remote(
            acc.at[sx, pl.ds(2 * sp, 2), slot("y", p2), rows], r2.at[sx, pl.ds(2 * sp, 2), rows],
            s2s, s2r.at[index, t], peer("y", p2),
        )

    def multiply(t, rel):
        product = jnp.dot(ct[rel], abuf[t], preferred_element_type=F32)
        product = product.astype(jnp.bfloat16).astype(F32)
        for hrel in (0, 1):
            for n in range(4):
                yield n // 2, slot("y", 2 * hrel + n % 2), product[hrel * 256 : hrel * 256 + 256, n * 128 : n * 128 + 128]

    def for_other(t):
        pltpu.make_async_copy(abuf.at[t], abuf.at[t], a_sem.at[t]).wait()
        for n, target, block in multiply(t, 1):
            dsend[t, n, target] = block
        d2d(t).start()

    def own(t):
        sx, sp = t // 2, t % 2
        with jax.named_scope("d2dwait"):
            d2d(t).wait_recv()
        with jax.named_scope("dotown"):
            for n, target, block in multiply(t, 0):
                acc[sx, 2 * sp + n, target] = block + drecv[t, n, target]
        for c in xs:
            for i, k in ((0, 2), (1, c[2])):

                @pl.when(sx == slot("x", k))
                def _(c=c, i=i):
                    x_send1(c, sx, sp, i).start()

        for c in zs:
            for i, k in ((0, 2), (1, c[2])):
                sz = slot("z", k)

                @pl.when(sp == sz // 2)
                def _(c=c, i=i, sz=sz):
                    z_send1(c, sx, sz, i).start()

        for c in ys:
            for n in (0, 1):
                y_send1(c, t, sx, sp, n).start()

    def second(t):
        sx, sp = t // 2, t % 2
        for c in xs:
            p2, rows = c[3], c[4]

            @pl.when(sx == slot("x", p2))
            def _(c=c, rows=rows):
                x_send1(c, sx, sp, 0).wait_recv()
                acc[sx, pl.ds(2 * sp, 2), :, rows] = acc[sx, pl.ds(2 * sp, 2), :, rows] + r1[pl.ds(2 * sp, 2), :, rows]
                x_send2(c, sx, sp).start()

        for c in zs:
            p2, rows = c[3], c[4]

            @pl.when(sp == 1)
            def _(c=c, p2=p2, rows=rows):
                on = slot("z", p2)
                z_send1(c, sx, on, 0).wait_recv()
                acc[sx, on, :, rows] = acc[sx, on, :, rows] + r1[sx, :, rows]
                z_send2(c, sx, on).start()

        for c in ys:
            _, _, p1, p2, rows = c
            on = slot("y", p2)
            y_wait1(c, t)
            for n in (0, 1):
                sz = 2 * sp + n
                acc[sx, sz, on, rows] = acc[sx, sz, on, rows] + r1[t, n * 2 + pair_item(p1, False), rows]
                acc[sx, sz, KEEP, rows] = acc[sx, sz, KEEP, rows] + r1[t, n * 2 + pair_item(p1, True), rows]
            y_send2(c, t, sx, sp).start()

    def step(u, carry):
        @pl.when(u < 8)
        def _():
            with jax.named_scope("dotsend"):
                for_other(u)

        @pl.when(u == 0)
        def _():
            transpose(0)

        @pl.when((u >= LAG1) & (u < 8 + LAG1))
        def _():
            own(u - LAG1)

        @pl.when(u >= LAG2)
        def _():
            with jax.named_scope("second"):
                second(u - LAG2)

        return carry

    lax.fori_loop(0, 8 + LAG2, step, 0)

    def x_send3(c, sz):
        index, _, p1, _, rows = c
        return remote(
            acc.at[3, sz, pl.ds(pair_start(p1), 2), rows], r3.at[pl.ds(sz * 2, 2), rows], s3s, s3r.at[index, sz], peer("y", p1)
        )

    def y_send3(c, sx):
        index, _, p1, _, rows = c
        return remote(
            acc.at[sx, pl.ds(pair_start(p1), 2), KEEP, rows], r3.at[pl.ds(sx * 2, 2), rows],
            s3s, s3r.at[index, sx], peer("z", p1),
        )

    def z_send3(c, i):
        index, _, p1, _, rows = c
        sx = slot("x", (2, p1)[i])
        return remote(acc.at[sx, KEEP, :, rows], r3.at[pl.ds(i * 4, 4), rows], s3s, s3r.at[index, i], peer("x", p1))

    with jax.named_scope("x3"):
        for sp in (0, 1):
            for c in xs:
                rows = c[4]
                x_send1(c, 0, sp, 1).wait_recv()
                x_send2(c, 0, sp).wait_recv()
                for sz in (2 * sp, 2 * sp + 1):
                    acc[3, sz, :, rows] = acc[3, sz, :, rows] + (r1[4 + sz, :, rows] + r2[sz, :, rows])
                    x_send3(c, sz).start()

    with jax.named_scope("zy3"):
        for sx in range(4):
            for c in zs:
                _, _, p1, _, rows = c
                z_send1(c, sx, 0, 1).wait_recv()
                z_send2(c, sx, 0).wait_recv()
                acc[sx, 3, :, rows] = acc[sx, 3, :, rows] + (r1[4 + sx, :, rows] + r2[sx, :, rows])
                for i in (0, 1):
                    if sx == slot("x", (2, p1)[i]):
                        z_send3(c, i).start()
            for c in ys:
                rows = c[4]
                for sp in (0, 1):
                    y_send2(c, sx * 2 + sp, sx, sp).wait_recv()
                acc[sx, :, KEEP, rows] = acc[sx, :, KEEP, rows] + r2[sx, :, rows]
                y_send3(c, sx).start()

    def x_send4(c):
        index, _, _, p2, rows = c
        return remote(acc.at[3, :, slot("y", p2), rows], r4.at[:, rows], s4s, s4r.at[index], peer("y", p2))

    def y_send4(c):
        index, _, _, p2, rows = c
        return remote(acc.at[:, slot("z", p2), KEEP, rows], r4.at[:, rows], s4s, s4r.at[index], peer("z", p2))

    def z_send4(c):
        index, _, _, p2, rows = c
        return remote(acc.at[slot("x", p2), KEEP, :, rows], r4.at[:, rows], s4s, s4r.at[index], peer("x", p2))

    with jax.named_scope("x4"):
        for c in xs:
            _, _, p1, p2, rows = c
            on = slot("y", p2)
            for sz in range(4):
                x_send3(c, sz).wait_recv()
                acc[3, sz, on, rows] = acc[3, sz, on, rows] + r3[sz * 2 + pair_item(p1, False), rows]
                acc[3, sz, KEEP, rows] = acc[3, sz, KEEP, rows] + r3[sz * 2 + pair_item(p1, True), rows]
            x_send4(c).start()
    with jax.named_scope("z4"):
        for c in zs:
            _, _, p1, p2, rows = c
            on = slot("x", p2)
            z_send3(c, 0).wait_recv()
            acc[on, KEEP, :, rows] = acc[on, KEEP, :, rows] + r3[pl.ds(0, 4), rows]
            z_send4(c).start()
    with jax.named_scope("y4"):
        for c in ys:
            _, _, p1, p2, rows = c
            on = slot("z", p2)
            for sx in range(4):
                y_send3(c, sx).wait_recv()
                acc[sx, on, KEEP, rows] = acc[sx, on, KEEP, rows] + r3[sx * 2 + pair_item(p1, False), rows]
                acc[sx, 3, KEEP, rows] = acc[sx, 3, KEEP, rows] + r3[sx * 2 + pair_item(p1, True), rows]
            y_send4(c).start()

    def x_send5(c):
        index, _, p1, _, rows = c
        return remote(
            acc.at[3, pl.ds(pair_start(p1), 2), KEEP, rows], r5.at[:, rows], s5s, s5r.at[index, 0], peer("z", p1)
        )

    def z_send5(c):
        index, _, p1, _, rows = c
        return remote(
            acc.at[3, KEEP, pl.ds(pair_start(p1), 2), rows], r5.at[:, rows], s5s, s5r.at[index, 0], peer("y", p1)
        )

    def y_send5(c, i):
        index, _, p1, _, rows = c
        return remote(
            acc.at[slot("x", (2, p1)[i]), KEEP, KEEP, rows], r5.at[i, rows], s5s, s5r.at[index, i], peer("x", p1)
        )

    with jax.named_scope("x5"):
        for c in xs:
            rows = c[4]
            x_send4(c).wait_recv()
            acc[3, :, KEEP, rows] = acc[3, :, KEEP, rows] + r4[:, rows]
            x_send5(c).start()
    with jax.named_scope("z5"):
        for c in zs:
            _, _, p1, _, rows = c
            z_send3(c, 1).wait_recv()
            z_send4(c).wait_recv()
            acc[3, KEEP, :, rows] = acc[3, KEEP, :, rows] + (r3[pl.ds(4, 4), rows] + r4[:, rows])
            z_send5(c).start()
    with jax.named_scope("y5"):
        for c in ys:
            rows = c[4]
            y_send4(c).wait_recv()
            acc[:, 3, KEEP, rows] = acc[:, 3, KEEP, rows] + r4[:, rows]
            for i in (0, 1):
                y_send5(c, i).start()

    def last(c, axis):
        index, _, _, p2, rows = c
        on = slot(axis, p2)
        src = {"x": acc.at[on, KEEP, KEEP, rows], "y": acc.at[3, KEEP, on, rows], "z": acc.at[3, on, KEEP, rows]}[axis]
        return remote(src, r6.at[rows], s6s, s6r.at[index], peer(axis, p2))

    def to_far(c):
        index, rows = c[0], c[4]
        return remote(acc.at[3, KEEP, KEEP, rows], afar.at[rows], fs_sem, fr_sem.at[index], far)

    groups = ((xs, "z"), (zs, "y"), (ys, "x"))
    for group, axis in groups:
        with jax.named_scope("last" + axis):
            for c in group:
                _, _, p1, p2, rows = c
                on = slot(axis, p2)
                if axis == "x":
                    y_send5(c, 0).wait_recv()
                    y_send5(c, 1).wait_recv()
                    onward, kept = r5[0, rows], r5[1, rows]
                    acc[on, KEEP, KEEP, rows] = acc[on, KEEP, KEEP, rows] + onward
                else:
                    (x_send5 if axis == "z" else z_send5)(c).wait_recv()
                    onward, kept = r5[pair_item(p1, False), rows], r5[pair_item(p1, True), rows]
                    if axis == "z":
                        acc[3, on, KEEP, rows] = acc[3, on, KEEP, rows] + onward
                    else:
                        acc[3, KEEP, on, rows] = acc[3, KEEP, on, rows] + onward
                last(c, axis).start()
                acc[3, KEEP, KEEP, rows] = acc[3, KEEP, KEEP, rows] + kept

    for group, axis in groups:
        with jax.named_scope("far" + axis):
            for c in group:
                rows = c[4]
                last(c, axis).wait_recv()
                acc[3, KEEP, KEEP, rows] = acc[3, KEEP, KEEP, rows] + r6[rows]
                to_far(c).start()

    own_place = pl.ds(pl.multiple_of(yhi * 256, 256), 256)
    far_place = pl.ds(pl.multiple_of((1 - yhi) * 256, 256), 256)

    def swap(n, place):
        return remote(
            fin.at[n, pl.ds((1 - core) * 64, 64)], obuf.at[core, :, place], es_sem.at[n], er_sem.at[n], other_core
        )

    with jax.named_scope("swap0"):
        fin[0] = acc[3, KEEP, KEEP].T
        swap(0, own_place).start()
        obuf[core, :, own_place] = fin[0, pl.ds(core * 64, 64)]
    with jax.named_scope("farwait"):
        for c in cols:
            to_far(c).wait_recv()
    with jax.named_scope("swap1"):
        fin[1] = afar[...].T
        swap(1, far_place).start()
        obuf[core, :, far_place] = fin[1, pl.ds(core * 64, 64)]
        swap(0, own_place).wait_recv()
        swap(1, far_place).wait_recv()
        out_k[...] = obuf[0]
        out_v[...] = obuf[1]

    with jax.named_scope("ends"):
        for whole, sem in (
            (drecv, ds_sem), (r1, s1s), (r2, s2s), (r3, s3s), (r4, s4s), (r5, s5s), (r6, s6s), (afar, fs_sem)
        ):
            remote(whole, whole, sem, er_sem.at[0], other_core).wait_send()
        for n, place in ((0, own_place), (1, far_place)):
            swap(n, place).wait_send()


def local(activations, key_cotangent, value_cotangent):
    tok, width = activations.shape
    half = key_cotangent.shape[1]
    rows = width // 64
    dma = pltpu.SemaphoreType.DMA
    return pl.pallas_call(
        kernel,
        out_shape=(jax.ShapeDtypeStruct((rows, half), F32), jax.ShapeDtypeStruct((rows, half), F32)),
        in_specs=[pl.BlockSpec(memory_space=pl.ANY)] * 3,
        out_specs=(pl.BlockSpec(memory_space=pltpu.VMEM), pl.BlockSpec(memory_space=pltpu.VMEM)),
        scratch_shapes=[
            pltpu.VMEM((8, tok, 512), jnp.bfloat16),
            pltpu.VMEM((2, 2, tok, 256), jnp.bfloat16),
            pltpu.VMEM((2, 512, tok), jnp.bfloat16),
            pltpu.VMEM((4, 4, 4, 256, 128), F32),
            pltpu.VMEM((8, 2, 4, 256, 128), F32),
            pltpu.VMEM((8, 2, 4, 256, 128), F32),
            pltpu.VMEM((8, 4, 256, 128), F32),
            pltpu.VMEM((4, 4, 256, 128), F32),
            pltpu.VMEM((8, 256, 128), F32),
            pltpu.VMEM((4, 256, 128), F32),
            pltpu.VMEM((2, 256, 128), F32),
            pltpu.VMEM((256, 128), F32),
            pltpu.VMEM((256, 128), F32),
            pltpu.VMEM((2, 128, 256), F32),
            pltpu.VMEM((2, rows, half), F32),
            dma((8,)), dma((2, 2)), dma, dma((8,)),
            dma, dma((6, 8)), dma, dma((6, 8)),
            dma, dma((6, 4)), dma, dma((6,)),
            dma, dma((6, 2)), dma, dma((6,)),
            dma, dma((6,)), dma((2,)), dma((2,)),
        ],
        compiler_params=pltpu.CompilerParams(
            collective_id=0, has_side_effects=True, vmem_limit_bytes=67_043_328
        ),
        name="weight_gradients",
    )(activations, key_cotangent, value_cotangent)


def solution(mesh):
    finer = Mesh(mesh.devices.reshape(mesh.shape["inter"], 4, 2, 4, 2), AXES)
    spec = P(AXES, None)
    out = P(INTRA, None)
    return jax.shard_map(local, mesh=finer, in_specs=(spec, spec, spec), out_specs=(out, out), check_vma=False)
```

```python
import jax
import jax.numpy as jnp
from jax import lax
from jax.experimental import pallas as pl
from jax.experimental.pallas import tpu as pltpu
from jax.sharding import Mesh
from jax.sharding import PartitionSpec as P

MESH = pl.DeviceIdType.MESH
F32 = jnp.float32
AXES = ("inter", "x", "ylo", "z", "core")
INTRA = ("x", "ylo", "z", "core")

UNIT_ORDER = (2, 0, 1, 3)
ORDER = (1, 2, 3, 0)
KEEP = 3
SIZES = ((24, 16, 24, 24, 16, 24), (16, 24, 24, 16, 24, 24))
LAG1 = 2
LAG2 = 5


def flip(r, k):
    if k == 0:
        return r
    if k == 1:
        return r + 1 - 2 * (r % 2)
    if k == 2:
        return (r + 2) % 4
    return 3 - r


def colours(wave):
    result, off = [], 0
    for order in ("yzx", "xyz", "zxy"):
        for p1, p2 in ((1, 3), (3, 1)):
            size = SIZES[wave][len(result)]
            result.append((len(result), order, p1, p2, pl.ds(off, size)))
            off += size
    return result


def pair_start(p1):
    return 0 if p1 == 1 else 1


def onward_item(p1):
    return 1 if p1 == 1 else 0


def kept_item(p1):
    return 1 - onward_item(p1)


def unit_at(sx, sz):
    return (sx // 2) * 4 + (sz // 2) * 2 + (sx + sz) % 2, sx % 2


def kernel(
    a_hbm, k_hbm, v_hbm, out,
    abuf, cst, ct, acc, dsend, drecv, r1, r1y, r2, b2, r3, r4, fin, obuf,
    a_sem, c_sem, ds_sem, dr_sem, s1s, s1r, s2s, s2r, s3s, s3r, s4s, s4r, es_sem, er_sem,
):
    x, z = lax.axis_index("x"), lax.axis_index("z")
    yhi, ylo = lax.axis_index("inter"), lax.axis_index("ylo")
    core = lax.axis_index("core")
    y = 2 * yhi + ylo

    def peer(axis, k):
        if axis == "x":
            return {"x": flip(x, k)}
        if axis == "z":
            return {"z": flip(z, k)}
        to = flip(y, k)
        return {"inter": to // 2, "ylo": to % 2}

    other_core = {"core": 1 - core}
    far = {"inter": 1 - yhi}
    far_other = {"inter": 1 - yhi, "core": 1 - core}

    barrier = pltpu.get_barrier_semaphore()
    peers = [other_core, far_other] + [peer(axis, k) for axis in "xyz" for k in (1, 2, 3)]
    for device in peers:
        pl.semaphore_signal(barrier, inc=1, device_id=device, device_id_type=MESH)

    def c_start(wave, priority):
        for which, src in ((0, k_hbm), (1, v_hbm)):
            rel = core if which == 0 else 1 - core
            for hrel in (0, 1):
                half = (yhi + hrel) % 2
                pltpu.make_async_copy(
                    src.at[:, pl.ds(pl.multiple_of(half * 256 + wave * 128, 128), 128)], cst.at[wave, rel, hrel], c_sem.at[wave]
                ).start(priority=priority)

    def c_wait(wave):
        pltpu.make_async_copy(cst.at[wave], cst.at[wave], c_sem.at[wave]).wait()

    def a_start(t, priority):
        for n in (0, 1):
            tx, tz = flip(x, UNIT_ORDER[t // 4 * 2 + n]), flip(z, UNIT_ORDER[t // 2 % 2 * 2 + (n + t) % 2])
            for lrel in (0, 1):
                column = pl.multiple_of(((tx * 2 + (ylo + lrel) % 2) * 4 + tz) * 128, 128)
                pltpu.make_async_copy(
                    a_hbm.at[:, pl.ds(column, 128)], abuf.at[t, :, pl.ds((n * 2 + lrel) * 128, 128)], a_sem.at[t]
                ).start(priority=priority)

    with jax.named_scope("cwait"):
        c_start(0, 0)
        a_start(0, 0)
        a_start(1, 1)
        c_start(1, 1)
        for t in range(2, 8):
            a_start(t, 1)
        c_wait(0)

    def transpose(rel, wave):
        for hrel in (0, 1):
            ct[rel, wave, pl.ds(hrel * 128, 128), :] = cst[wave, rel, hrel].T

    with jax.named_scope("ctrans"):
        transpose(1, 0)

    def remote(src, dst, send, recv, device):
        return pltpu.make_async_remote_copy(
            src_ref=src, dst_ref=dst, send_sem=send, recv_sem=recv, device_id=device, device_id_type=MESH
        )

    def d2d(g):
        return remote(dsend.at[g], drecv.at[g], ds_sem, dr_sem.at[g % 4], other_core)

    def first_sem(c, w, which):
        index = c[0]
        return s1r.at[w, index * 8 + which] if index < 2 else s1r.at[w, 16 + (index - 2) * 3 + which]

    def send1(c, w, t):
        index, order, p1, _, rows = c
        xt, zt, m = t // 4, t // 2 % 2, t % 2
        device = peer(order[0], p1)
        if order[0] == "y":
            return remote(
                acc.at[w, t, :, pl.ds(pair_start(p1), 2), rows], r1y.at[w, t, :, :, rows], s1s, first_sem(c, w, t), device
            )
        if order[0] == "x":
            n = 0 if p1 == 1 else xt
            item = xt * 4 + zt * 2 + (n + m) % 2
            sem = first_sem(c, w, 2 * xt)
        else:
            n = m if p1 == 1 else (m + zt) % 2
            item = zt * 4 + xt * 2 + n
            sem = first_sem(c, w, xt + zt * (2 - xt))
        return remote(acc.at[w, t, n, :, rows], r1.at[w, item, :, rows], s1s, sem, device)

    def wait_for(ref, sem):
        remote(ref, ref, s1s, sem, other_core).wait_recv()

    def send2(c, w, t, n, item):
        index, order, _, p2, rows = c
        device = peer(order[0], p2)
        if order[0] == "y":
            return remote(
                acc.at[w, t, :, ORDER.index(p2), rows], r2.at[w, t // 2, pl.ds(t % 2 * 2, 2), rows], s2s, s2r.at[w, index], device
            )
        return remote(acc.at[w, t, n, :, rows], r2.at[w, item, :, rows], s2s, s2r.at[w, index], device)

    def multiply(t, w, rel):
        product = jnp.dot(ct[rel, w], abuf[t], preferred_element_type=F32)
        product = product.astype(jnp.bfloat16).astype(F32)
        for hrel in (0, 1):
            for n in (0, 1):
                for lrel in (0, 1):
                    place = (n * 2 + lrel) * 128
                    yield n, ORDER.index(2 * hrel + lrel), product[hrel * 128 : hrel * 128 + 128, place : place + 128]

    def a_wait(g):
        pltpu.make_async_copy(abuf.at[g], abuf.at[g], a_sem.at[g]).wait()

    def for_other(g):
        for n, target, block in multiply(g % 8, g // 8, 1):
            dsend[g, n, target] = block

    def own(g):
        for n, target, block in multiply(g % 8, g // 8, 0):
            acc[g // 8, g % 8, n, target] = block + drecv[g, n, target]

    def first(g):
        for wave in (0, 1):

            @pl.when(g // 8 == wave)
            def _(wave=wave):
                for c in colours(wave):
                    send1(c, wave, g % 8).start()

    def second(w, t):
        xt, zt, m = t // 4, t // 2 % 2, t % 2

        def onward(c, n, item):
            rows = c[4]
            acc[w, t, n, :, rows] = acc[w, t, n, :, rows] + r1[w, item, :, rows]
            send2(c, w, t, n, item).start()

        ys, xs, zs = colours(w)[0:2], colours(w)[2:4], colours(w)[4:6]
        for c in ys:
            _, _, p1, p2, rows = c
            on = ORDER.index(p2)
            send1(c, w, t).wait_recv()
            for n in (0, 1):
                acc[w, t, n, on, rows] = acc[w, t, n, on, rows] + r1y[w, t, n, onward_item(p1), rows]
            send2(c, w, t, 0, 0).start()

        @pl.when(t == 4)
        def _():
            for c in xs:
                wait_for(r1.at[w, pl.ds(0, 4), :, c[4]], first_sem(c, w, 0))

        @pl.when((zt == 1) & (m == 0))
        def _():
            for c in zs:
                wait_for(r1.at[w, pl.ds(0, 2), :, c[4]], first_sem(c, w, xt))

        @pl.when(xt == 1)
        def _():
            for c in xs:
                n = 1 if c[2] == 1 else 0
                onward(c, n, zt * 2 + (n + m) % 2)

        @pl.when(zt == 1)
        def _():
            for c in zs:
                n = 1 - m if c[2] == 1 else m
                onward(c, n, xt * 2 + n)

    def stage1(w):
        for c in colours(w)[2:6]:
            index, order, p1, _, rows = c
            wait_for(r1.at[w, pl.ds(4, 4), :, rows], first_sem(c, w, 2))
            wait_for(r2.at[w, :, :, rows], s2r.at[w, index])
            for item in range(4):
                t, n = unit_at(1, item) if order[0] == "x" else unit_at(item, 1)
                total = acc[w, t, n, :, rows] + (r1[w, 4 + item, :, rows] + r2[w, item, :, rows])
                place = ORDER.index(UNIT_ORDER[item])
                if order[0] == "x":
                    b2[w, :, place, rows] = total
                else:
                    b2[w, place, :, rows] = total
            spread2(c, w)
        for c in colours(w)[0:2]:
            index, _, p1, _, rows = c
            wait_for(r2.at[w, :, :, rows], s2r.at[w, index])
            for sx in range(4):
                for sz in range(4):
                    t, n = unit_at(sx, sz)
                    total = acc[w, t, n, KEEP, rows] + (r1y[w, t, n, kept_item(p1), rows] + r2[w, t // 2, t % 2 * 2 + n, rows])
                    b2[w, ORDER.index(UNIT_ORDER[sz]), ORDER.index(UNIT_ORDER[sx]), rows] = total
            spread2(c, w)

    def spread2(c, w):
        index, order, _, _, rows = c
        for n, k in enumerate(ORDER[:3]):
            remote(b2.at[w, n, :, rows], r3.at[w, n, :, rows], s3s, s3r.at[w, index], peer(order[1], k)).start()

    def spread3(c, w):
        index, order, _, _, rows = c
        for n, k in enumerate(ORDER[:3]):
            remote(b2.at[w, KEEP, n, rows], r4.at[w, n, rows], s4s, s4r.at[w, index], peer(order[2], k)).start()

    def in_order(w):
        every = colours(w)
        return every[2:6] + every[0:2]

    def stage2(w):
        for c in in_order(w):
            index, rows = c[0], c[4]
            wait_for(r3.at[w, :, :, rows], s3r.at[w, index])
            b2[w, KEEP, :, rows] = (b2[w, KEEP, :, rows] + r3[w, 0, :, rows]) + (r3[w, 1, :, rows] + r3[w, 2, :, rows])
            spread3(c, w)

    def stage3(w):
        for c in in_order(w):
            index, rows = c[0], c[4]
            wait_for(r4.at[w, :, rows], s4r.at[w, index])
            b2[w, KEEP, KEEP, rows] = (b2[w, KEEP, KEEP, rows] + r4[w, 0, rows]) + (r4[w, 1, rows] + r4[w, 2, rows])

    def spread4(w, n):
        to_core, device = ((core, far), (1 - core, far_other), (1 - core, other_core))[n]
        return remote(
            fin.at[w, pl.ds(to_core * 64, 64)],
            obuf.at[core, :, pl.ds(pl.multiple_of(yhi * 256 + w * 128, 128), 128)],
            es_sem, er_sem.at[w, n], device,
        )

    def stage4(w):
        fin[w] = b2[w, KEEP, KEEP].T
        for n in range(3):
            spread4(w, n).start()
        obuf[core, :, pl.ds(pl.multiple_of(yhi * 256 + w * 128, 128), 128)] = fin[w, pl.ds(core * 64, 64)]

    with jax.named_scope("start"):
        a_wait(0)
        for_other(0)
        pl.semaphore_wait(barrier, len(peers))
        d2d(0).start()
        transpose(0, 0)
        a_wait(1)
        for_other(1)
        d2d(1).start()

    def step(g, carry):
        @pl.when(g < 8)
        def _():
            a_wait(g)

        with jax.named_scope("d2dwait"):
            d2d(g - LAG1).wait_recv()
        with jax.named_scope("dots"):
            for_other(g)
            own(g - LAG1)
        d2d(g).start()
        first(g - LAG1)

        @pl.when(g == 3)
        def _():
            c_wait(1)
            transpose(1, 1)
            transpose(0, 1)

        for wave in (0, 1):

            @pl.when((g >= LAG2 + 8 * wave) & (g < LAG2 + 8 * wave + 8))
            def _(wave=wave):
                with jax.named_scope("second"):
                    second(wave, g - LAG2 - 8 * wave)

        return carry

    lax.fori_loop(LAG1, 16, step, 0)

    for g in range(16, 16 + LAG2):
        if g < 16 + LAG1:
            with jax.named_scope("own"):
                d2d(g - LAG1).wait_recv()
                own(g - LAG1)
                for c in colours(1):
                    send1(c, 1, g - LAG1 - 8).start()
        with jax.named_scope("second"):
            second(1, g - LAG2 - 8)
        if g == 17:
            with jax.named_scope("e1"):
                stage1(0)

    for name, stage, w in (
        ("f1", stage1, 1), ("e2", stage2, 0), ("f2", stage2, 1), ("e3", stage3, 0), ("e4", stage4, 0),
        ("f3", stage3, 1), ("f4", stage4, 1),
    ):
        with jax.named_scope(name):
            stage(w)

    with jax.named_scope("swapwait"):
        for w in (0, 1):
            for n in range(3):
                spread4(w, n).wait_recv()
        out[...] = obuf[...]

    with jax.named_scope("ends"):
        for wave in (0, 1):
            rest = colours(wave)[2:6]
            for whole in (
                r1y.at[wave, :, :, :, pl.ds(0, SIZES[wave][0] + SIZES[wave][1])],
                r1.at[wave, :, :, pl.ds(rest[0][4].start, 128 - rest[0][4].start)],
            ):
                remote(whole, whole, s1s, er_sem.at[0, 0], other_core).wait_send()
        for whole, sem in (
            (drecv, ds_sem), (r2, s2s), (r3, s3s), (r4, s4s), (drecv.at[0, 0, pl.ds(0, 3)], es_sem)
        ):
            remote(whole, whole, sem, er_sem.at[0, 0], other_core).wait_send()


def local(activations, key_cotangent, value_cotangent):
    tok, width = activations.shape
    half = key_cotangent.shape[1]
    rows = width // 64
    y_rows = max(sizes[0] + sizes[1] for sizes in SIZES)
    dma = pltpu.SemaphoreType.DMA
    both = pl.pallas_call(
        kernel,
        out_shape=jax.ShapeDtypeStruct((2, rows, half), F32),
        in_specs=[pl.BlockSpec(memory_space=pl.ANY)] * 3,
        out_specs=pl.BlockSpec(memory_space=pltpu.VMEM),
        scratch_shapes=[
            pltpu.VMEM((8, tok, 512), jnp.bfloat16),
            pltpu.VMEM((2, 2, 2, tok, 128), jnp.bfloat16),
            pltpu.VMEM((2, 2, 256, tok), jnp.bfloat16),
            pltpu.VMEM((2, 8, 2, 4, 128, 128), F32),
            pltpu.VMEM((16, 2, 4, 128, 128), F32),
            pltpu.VMEM((16, 2, 4, 128, 128), F32),
            pltpu.VMEM((2, 8, 4, 128, 128), F32),
            pltpu.VMEM((2, 8, 2, 2, y_rows, 128), F32),
            pltpu.VMEM((2, 4, 4, 128, 128), F32),
            pltpu.VMEM((2, 4, 4, 128, 128), F32),
            pltpu.VMEM((2, 3, 4, 128, 128), F32),
            pltpu.VMEM((2, 3, 128, 128), F32),
            pltpu.VMEM((2, 128, 128), F32),
            pltpu.VMEM((2, rows, half), F32),
            dma((8,)), dma((2,)), dma, dma((4,)),
            dma, dma((2, 28)), dma, dma((2, 6)),
            dma, dma((2, 6)), dma, dma((2, 6)),
            dma, dma((2, 3)),
        ],
        compiler_params=pltpu.CompilerParams(
            collective_id=0, has_side_effects=True, vmem_limit_bytes=67_043_328
        ),
        name="weight_gradients",
    )(activations, key_cotangent, value_cotangent)
    return both[0], both[1]


def solution(mesh):
    finer = Mesh(mesh.devices.reshape(mesh.shape["inter"], 4, 2, 4, 2), AXES)
    spec = P(AXES, None)
    out = P(INTRA, None)
    return jax.shard_map(local, mesh=finer, in_specs=(spec, spec, spec), out_specs=(out, out), check_vma=False)
```

```python
import jax
import jax.numpy as jnp
from jax import lax
from jax.experimental import pallas as pl
from jax.experimental.pallas import tpu as pltpu
from jax.sharding import Mesh
from jax.sharding import PartitionSpec as P

MESH = pl.DeviceIdType.MESH
F32 = jnp.float32
AXES = ("inter", "x", "ylo", "z", "core")
INTRA = ("x", "ylo", "z", "core")

UNIT_ORDER = (2, 0, 1, 3)
ORDER = (1, 2, 3, 0)
KEEP = 3
LIMIT = 52 * 1024 * 1024
FAR_FIRST = (1, 0, 2)
SIZES = ((24, 16, 24, 24, 16, 24), (16, 24, 24, 16, 24, 24))
LAG1 = 2
LAG2 = 5


def flip(r, k):
    if k == 0:
        return r
    if k == 1:
        return r + 1 - 2 * (r % 2)
    if k == 2:
        return (r + 2) % 4
    return 3 - r


def colours(wave):
    result, off = [], 0
    for order in ("yzx", "xyz", "zxy"):
        for p1, p2 in ((1, 3), (3, 1)):
            size = SIZES[wave][len(result)]
            result.append((len(result), order, p1, p2, pl.ds(off, size)))
            off += size
    return result


def pair_start(p1):
    return 0 if p1 == 1 else 1


def onward_item(p1):
    return 1 if p1 == 1 else 0


def kept_item(p1):
    return 1 - onward_item(p1)


def unit_at(sx, sz):
    return (sx // 2) * 4 + (sz // 2) * 2 + (sx + sz) % 2, sx % 2


def kernel(
    a_hbm, k_hbm, v_hbm, out,
    abuf, cst, ct, acc, dsend, drecv, r1, r1y, r2, b2, r3, r4, fin, obuf,
    a_sem, c_sem, ds_sem, dr_sem, s1s, s1r, s2s, s2r, s3s, s3r, s4s, s4r, es_sem, er_sem,
):
    x, z = lax.axis_index("x"), lax.axis_index("z")
    yhi, ylo = lax.axis_index("inter"), lax.axis_index("ylo")
    core = lax.axis_index("core")
    y = 2 * yhi + ylo

    def peer(axis, k):
        if axis == "x":
            return {"x": flip(x, k)}
        if axis == "z":
            return {"z": flip(z, k)}
        to = flip(y, k)
        return {"inter": to // 2, "ylo": to % 2}

    other_core = {"core": 1 - core}
    far = {"inter": 1 - yhi}
    far_other = {"inter": 1 - yhi, "core": 1 - core}

    barrier = pltpu.get_barrier_semaphore()
    peers = [other_core, far_other] + [peer(axis, k) for axis in "xyz" for k in (1, 2, 3)]
    for device in peers:
        pl.semaphore_signal(barrier, inc=1, device_id=device, device_id_type=MESH)

    def c_start(wave, priority):
        for which, src in ((0, k_hbm), (1, v_hbm)):
            rel = core if which == 0 else 1 - core
            for hrel in (0, 1):
                half = (yhi + hrel) % 2
                pltpu.make_async_copy(
                    src.at[:, pl.ds(pl.multiple_of(half * 256 + wave * 128, 128), 128)], cst.at[wave, rel, hrel], c_sem.at[wave]
                ).start(priority=priority)

    def c_wait(wave):
        pltpu.make_async_copy(cst.at[wave], cst.at[wave], c_sem.at[wave]).wait()

    def a_start(t, priority):
        for n in (0, 1):
            tx, tz = flip(x, UNIT_ORDER[t // 4 * 2 + n]), flip(z, UNIT_ORDER[t // 2 % 2 * 2 + (n + t) % 2])
            for lrel in (0, 1):
                column = pl.multiple_of(((tx * 2 + (ylo + lrel) % 2) * 4 + tz) * 128, 128)
                pltpu.make_async_copy(
                    a_hbm.at[:, pl.ds(column, 128)], abuf.at[t, :, pl.ds((n * 2 + lrel) * 128, 128)], a_sem.at[t]
                ).start(priority=priority)

    with jax.named_scope("cwait"):
        c_start(0, 0)
        a_start(0, 0)
        a_start(1, 1)
        c_start(1, 1)
        for t in range(2, 8):
            a_start(t, 1)
        c_wait(0)

    def transpose(rel, wave):
        for hrel in (0, 1):
            ct[rel, wave, pl.ds(hrel * 128, 128), :] = cst[wave, rel, hrel].T

    with jax.named_scope("ctrans"):
        transpose(1, 0)

    def remote(src, dst, send, recv, device):
        return pltpu.make_async_remote_copy(
            src_ref=src, dst_ref=dst, send_sem=send, recv_sem=recv, device_id=device, device_id_type=MESH
        )

    def d2d(g):
        return remote(dsend.at[g % 4], drecv.at[g % 4], ds_sem.at[g % 4], dr_sem.at[g % 4], other_core)

    def first_sem(c, w, which):
        index = c[0]
        return s1r.at[w, index * 8 + which] if index < 2 else s1r.at[w, 16 + (index - 2) * 3 + which]

    def send1(c, w, t):
        index, order, p1, _, rows = c
        xt, zt, m = t // 4, t // 2 % 2, t % 2
        device = peer(order[0], p1)
        if order[0] == "y":
            return remote(
                acc.at[w, t, :, pl.ds(pair_start(p1), 2), rows], r1y.at[w, t, :, :, rows], s1s, first_sem(c, w, t), device
            )
        if order[0] == "x":
            n = 0 if p1 == 1 else xt
            item = xt * 4 + zt * 2 + (n + m) % 2
            sem = first_sem(c, w, 2 * xt)
        else:
            n = m if p1 == 1 else (m + zt) % 2
            item = zt * 4 + xt * 2 + n
            sem = first_sem(c, w, xt + zt * (2 - xt))
        return remote(acc.at[w, t, n, :, rows], r1.at[w, item, :, rows], s1s, sem, device)

    def wait_for(ref, sem):
        remote(ref, ref, s1s, sem, other_core).wait_recv()

    def send2(c, w, t, n, item):
        index, order, _, p2, rows = c
        device = peer(order[0], p2)
        if order[0] == "y":
            return remote(
                acc.at[w, t, :, ORDER.index(p2), rows], r2.at[w, t // 2, pl.ds(t % 2 * 2, 2), rows], s2s, s2r.at[w, index], device
            )
        return remote(acc.at[w, t, n, :, rows], r2.at[w, item, :, rows], s2s, s2r.at[w, index], device)

    def multiply(t, w, rel):
        product = jnp.dot(ct[rel, w], abuf[t], preferred_element_type=F32)
        product = product.astype(jnp.bfloat16).astype(F32)
        for hrel in (0, 1):
            for n in (0, 1):
                for lrel in (0, 1):
                    place = (n * 2 + lrel) * 128
                    yield n, ORDER.index(2 * hrel + lrel), product[hrel * 128 : hrel * 128 + 128, place : place + 128]

    def a_wait(g):
        pltpu.make_async_copy(abuf.at[g], abuf.at[g], a_sem.at[g]).wait()

    def for_other(g):
        for n, target, block in multiply(g % 8, g // 8, 1):
            dsend[g % 4, n, target] = block

    def own(g):
        for n, target, block in multiply(g % 8, g // 8, 0):
            acc[g // 8, g % 8, n, target] = block + drecv[g % 4, n, target]

    def first(g):
        for wave in (0, 1):

            @pl.when(g // 8 == wave)
            def _(wave=wave):
                for c in colours(wave):
                    send1(c, wave, g % 8).start()

    def second(w, t):
        xt, zt, m = t // 4, t // 2 % 2, t % 2

        def onward(c, n, item):
            rows = c[4]
            acc[w, t, n, :, rows] = acc[w, t, n, :, rows] + r1[w, item, :, rows]
            send2(c, w, t, n, item).start()

        ys, xs, zs = colours(w)[0:2], colours(w)[2:4], colours(w)[4:6]
        for c in ys:
            _, _, p1, p2, rows = c
            on = ORDER.index(p2)
            send1(c, w, t).wait_recv()
            for n in (0, 1):
                acc[w, t, n, on, rows] = acc[w, t, n, on, rows] + r1y[w, t, n, onward_item(p1), rows]
            send2(c, w, t, 0, 0).start()

        @pl.when(t == 4)
        def _():
            for c in xs:
                wait_for(r1.at[w, pl.ds(0, 4), :, c[4]], first_sem(c, w, 0))

        @pl.when((zt == 1) & (m == 0))
        def _():
            for c in zs:
                wait_for(r1.at[w, pl.ds(0, 2), :, c[4]], first_sem(c, w, xt))

        @pl.when(xt == 1)
        def _():
            for c in xs:
                n = 1 if c[2] == 1 else 0
                onward(c, n, zt * 2 + (n + m) % 2)

        @pl.when(zt == 1)
        def _():
            for c in zs:
                n = 1 - m if c[2] == 1 else m
                onward(c, n, xt * 2 + n)

    def stage1(w):
        for c in colours(w)[2:6]:
            index, order, p1, _, rows = c
            wait_for(r1.at[w, pl.ds(4, 4), :, rows], first_sem(c, w, 2))
            wait_for(r2.at[w, :, :, rows], s2r.at[w, index])
            for item in range(4):
                t, n = unit_at(1, item) if order[0] == "x" else unit_at(item, 1)
                total = acc[w, t, n, :, rows] + (r1[w, 4 + item, :, rows] + r2[w, item, :, rows])
                place = ORDER.index(UNIT_ORDER[item])
                if order[0] == "x":
                    b2[w, :, place, rows] = total
                else:
                    b2[w, place, :, rows] = total
            spread2(c, w)
        for c in colours(w)[0:2]:
            index, _, p1, _, rows = c
            wait_for(r2.at[w, :, :, rows], s2r.at[w, index])
            for sx in range(4):
                for sz in range(4):
                    t, n = unit_at(sx, sz)
                    total = acc[w, t, n, KEEP, rows] + (r1y[w, t, n, kept_item(p1), rows] + r2[w, t // 2, t % 2 * 2 + n, rows])
                    b2[w, ORDER.index(UNIT_ORDER[sz]), ORDER.index(UNIT_ORDER[sx]), rows] = total
            spread2(c, w)

    def spread2(c, w):
        index, order, _, _, rows = c
        for n in FAR_FIRST:
            k = ORDER[n]
            remote(b2.at[w, n, :, rows], r3.at[w, n, :, rows], s3s, s3r.at[w, index], peer(order[1], k)).start()

    def spread3(c, w):
        index, order, _, _, rows = c
        for n in FAR_FIRST:
            k = ORDER[n]
            remote(b2.at[w, KEEP, n, rows], r4.at[w, n, rows], s4s, s4r.at[w, index], peer(order[2], k)).start()

    def in_order(w):
        every = colours(w)
        return every[2:6] + every[0:2]

    def stage2(w):
        for c in in_order(w):
            index, rows = c[0], c[4]
            wait_for(r3.at[w, :, :, rows], s3r.at[w, index])
            b2[w, KEEP, :, rows] = (b2[w, KEEP, :, rows] + r3[w, 0, :, rows]) + (r3[w, 1, :, rows] + r3[w, 2, :, rows])
            spread3(c, w)

    def stage3(w):
        for c in in_order(w):
            index, rows = c[0], c[4]
            wait_for(r4.at[w, :, rows], s4r.at[w, index])
            b2[w, KEEP, KEEP, rows] = (b2[w, KEEP, KEEP, rows] + r4[w, 0, rows]) + (r4[w, 1, rows] + r4[w, 2, rows])

    def spread4(w, n):
        to_core, device = ((core, far), (1 - core, far_other), (1 - core, other_core))[n]
        return remote(
            fin.at[w, pl.ds(to_core * 64, 64)],
            obuf.at[core, :, pl.ds(pl.multiple_of(yhi * 256 + w * 128, 128), 128)],
            es_sem, er_sem.at[w, n], device,
        )

    def stage4(w):
        fin[w] = b2[w, KEEP, KEEP].T
        for n in range(3):
            spread4(w, n).start()
        obuf[core, :, pl.ds(pl.multiple_of(yhi * 256 + w * 128, 128), 128)] = fin[w, pl.ds(core * 64, 64)]

    with jax.named_scope("start"):
        a_wait(0)
        for_other(0)
        transpose(0, 0)
        pl.semaphore_wait(barrier, len(peers))
        d2d(0).start()
        a_wait(1)
        for_other(1)
        d2d(1).start()

    def step(g, carry):
        @pl.when(g < 8)
        def _():
            a_wait(g)

        @pl.when(g >= 4)
        def _():
            d2d(g).wait_send()

        with jax.named_scope("d2dwait"):
            d2d(g - LAG1).wait_recv()
        with jax.named_scope("dots"):
            for_other(g)
            own(g - LAG1)
        d2d(g).start()
        first(g - LAG1)

        @pl.when(g == 3)
        def _():
            c_wait(1)
            transpose(1, 1)
            transpose(0, 1)

        for wave in (0, 1):

            @pl.when((g >= LAG2 + 8 * wave) & (g < LAG2 + 8 * wave + 8))
            def _(wave=wave):
                with jax.named_scope("second"):
                    second(wave, g - LAG2 - 8 * wave)

        return carry

    lax.fori_loop(LAG1, 16, step, 0)

    for g in range(16, 16 + LAG2):
        if g < 16 + LAG1:
            with jax.named_scope("own"):
                d2d(g - LAG1).wait_recv()
                own(g - LAG1)
                for c in colours(1):
                    send1(c, 1, g - LAG1 - 8).start()
        with jax.named_scope("second"):
            second(1, g - LAG2 - 8)
    for name, stage, w in (
        ("e1", stage1, 0), ("f1", stage1, 1), ("e2", stage2, 0), ("f2", stage2, 1), ("e3", stage3, 0), ("e4", stage4, 0),
        ("f3", stage3, 1), ("f4", stage4, 1),
    ):
        with jax.named_scope(name):
            stage(w)

    with jax.named_scope("swapwait"):
        for w in (0, 1):
            for n in range(3):
                spread4(w, n).wait_recv()
        out[...] = obuf[...]

    with jax.named_scope("ends"):
        for wave in (0, 1):
            rest = colours(wave)[2:6]
            for whole in (
                r1y.at[wave, :, :, :, pl.ds(0, SIZES[wave][0] + SIZES[wave][1])],
                r1.at[wave, :, :, pl.ds(rest[0][4].start, 128 - rest[0][4].start)],
            ):
                remote(whole, whole, s1s, er_sem.at[0, 0], other_core).wait_send()
        for whole, sem in (
            (r2, s2s), (r3, s3s), (r4, s4s), (r2.at[0, 0, pl.ds(0, 3)], es_sem)
        ):
            remote(whole, whole, sem, er_sem.at[0, 0], other_core).wait_send()
        for g in range(12, 16):
            d2d(g).wait_send()


def local(activations, key_cotangent, value_cotangent):
    tok, width = activations.shape
    half = key_cotangent.shape[1]
    rows = width // 64
    y_rows = max(sizes[0] + sizes[1] for sizes in SIZES)
    dma = pltpu.SemaphoreType.DMA
    both = pl.pallas_call(
        kernel,
        out_shape=jax.ShapeDtypeStruct((2, rows, half), F32),
        in_specs=[pl.BlockSpec(memory_space=pl.ANY)] * 3,
        out_specs=pl.BlockSpec(memory_space=pltpu.VMEM),
        scratch_shapes=[
            pltpu.VMEM((8, tok, 512), jnp.bfloat16),
            pltpu.VMEM((2, 2, 2, tok, 128), jnp.bfloat16),
            pltpu.VMEM((2, 2, 256, tok), jnp.bfloat16),
            pltpu.VMEM((2, 8, 2, 4, 128, 128), F32),
            pltpu.VMEM((4, 2, 4, 128, 128), F32),
            pltpu.VMEM((4, 2, 4, 128, 128), F32),
            pltpu.VMEM((2, 8, 4, 128, 128), F32),
            pltpu.VMEM((2, 8, 2, 2, y_rows, 128), F32),
            pltpu.VMEM((2, 4, 4, 128, 128), F32),
            pltpu.VMEM((2, 4, 4, 128, 128), F32),
            pltpu.VMEM((2, 3, 4, 128, 128), F32),
            pltpu.VMEM((2, 3, 128, 128), F32),
            pltpu.VMEM((2, 128, 128), F32),
            pltpu.VMEM((2, rows, half), F32),
            dma((8,)), dma((2,)), dma((4,)), dma((4,)),
            dma, dma((2, 28)), dma, dma((2, 6)),
            dma, dma((2, 6)), dma, dma((2, 6)),
            dma, dma((2, 3)),
        ],
        compiler_params=pltpu.CompilerParams(
            collective_id=0, has_side_effects=True, vmem_limit_bytes=LIMIT
        ),
        name="weight_gradients",
    )(activations, key_cotangent, value_cotangent)
    return both[0], both[1]


def solution(mesh):
    finer = Mesh(mesh.devices.reshape(mesh.shape["inter"], 4, 2, 4, 2), AXES)
    spec = P(AXES, None)
    out = P(INTRA, None)
    return jax.shard_map(local, mesh=finer, in_specs=(spec, spec, spec), out_specs=(out, out), check_vma=False)
```

```python
import jax
import jax.numpy as jnp
from jax import lax
from jax.experimental import pallas as pl
from jax.experimental.pallas import tpu as pltpu
from jax.sharding import Mesh
from jax.sharding import PartitionSpec as P

MESH = pl.DeviceIdType.MESH
F32 = jnp.float32
AXES = ("inter", "x", "ylo", "z", "core")
INTRA = ("x", "ylo", "z", "core")

UNIT_ORDER = (2, 0, 1, 3)
ORDER = (1, 2, 3, 0)
KEEP = 3
LIMIT = 52 * 1024 * 1024
FAR_FIRST = (1, 0, 2)
SIZES = ((24, 16, 24, 24, 16, 24), (16, 24, 24, 16, 24, 24))
LAG1 = 2
LAG2 = 5


def flip(r, k):
    if k == 0:
        return r
    if k == 1:
        return r + 1 - 2 * (r % 2)
    if k == 2:
        return (r + 2) % 4
    return 3 - r


def colours(wave):
    result, off = [], 0
    for order in ("yzx", "xyz", "zxy"):
        for p1, p2 in ((1, 3), (3, 1)):
            size = SIZES[wave][len(result)]
            result.append((len(result), order, p1, p2, pl.ds(off, size)))
            off += size
    return result


def pair_start(p1):
    return 0 if p1 == 1 else 1


def onward_item(p1):
    return 1 if p1 == 1 else 0


def kept_item(p1):
    return 1 - onward_item(p1)


def unit_at(sx, sz):
    return (sx // 2) * 4 + (sz // 2) * 2 + (sx + sz) % 2, sx % 2


def kernel(
    a_hbm, k_hbm, v_hbm, out,
    abuf, cst, ct, acc, dsend, drecv, r1, r1y, r2, b2, r3, r4, fin, obuf,
    a_sem, c_sem, ds_sem, dr_sem, s1s, s1r, s2s, s2r, s3s, s3r, s4s, s4r, es_sem, er_sem,
):
    x, z = lax.axis_index("x"), lax.axis_index("z")
    yhi, ylo = lax.axis_index("inter"), lax.axis_index("ylo")
    core = lax.axis_index("core")
    y = 2 * yhi + ylo

    def peer(axis, k):
        if axis == "x":
            return {"x": flip(x, k)}
        if axis == "z":
            return {"z": flip(z, k)}
        to = flip(y, k)
        return {"inter": to // 2, "ylo": to % 2}

    other_core = {"core": 1 - core}
    far = {"inter": 1 - yhi}
    far_other = {"inter": 1 - yhi, "core": 1 - core}

    barrier = pltpu.get_barrier_semaphore()
    peers = [other_core, far_other] + [peer(axis, k) for axis in "xyz" for k in (1, 2, 3)]
    for device in peers:
        pl.semaphore_signal(barrier, inc=1, device_id=device, device_id_type=MESH)

    def c_start(wave, priority):
        for which, src in ((0, k_hbm), (1, v_hbm)):
            rel = core if which == 0 else 1 - core
            for hrel in (0, 1):
                half = (yhi + hrel) % 2
                pltpu.make_async_copy(
                    src.at[:, pl.ds(pl.multiple_of(half * 256 + wave * 128, 128), 128)], cst.at[wave, rel, hrel], c_sem.at[wave]
                ).start(priority=priority)

    def c_wait(wave):
        pltpu.make_async_copy(cst.at[wave], cst.at[wave], c_sem.at[wave]).wait()

    def a_start(t, priority):
        for n in (0, 1):
            tx, tz = flip(x, UNIT_ORDER[t // 4 * 2 + n]), flip(z, UNIT_ORDER[t // 2 % 2 * 2 + (n + t) % 2])
            for lrel in (0, 1):
                column = pl.multiple_of(((tx * 2 + (ylo + lrel) % 2) * 4 + tz) * 128, 128)
                pltpu.make_async_copy(
                    a_hbm.at[:, pl.ds(column, 128)], abuf.at[t, :, pl.ds((n * 2 + lrel) * 128, 128)], a_sem.at[t]
                ).start(priority=priority)

    with jax.named_scope("cwait"):
        c_start(0, 0)
        a_start(0, 0)
        a_start(1, 1)
        c_start(1, 1)
        for t in range(2, 8):
            a_start(t, 1)
        c_wait(0)

    def transpose(rel, wave):
        for hrel in (0, 1):
            ct[rel, wave, pl.ds(hrel * 128, 128), :] = cst[wave, rel, hrel].T

    with jax.named_scope("ctrans"):
        transpose(1, 0)

    def remote(src, dst, send, recv, device):
        return pltpu.make_async_remote_copy(
            src_ref=src, dst_ref=dst, send_sem=send, recv_sem=recv, device_id=device, device_id_type=MESH
        )

    def d2d(g):
        return remote(dsend.at[g % 4], drecv.at[g % 4], ds_sem.at[g % 4], dr_sem.at[g % 4], other_core)

    def first_sem(c, w, which):
        index = c[0]
        return s1r.at[w, index * 8 + which] if index < 2 else s1r.at[w, 16 + (index - 2) * 3 + which]

    def send1(c, w, t):
        index, order, p1, _, rows = c
        xt, zt, m = t // 4, t // 2 % 2, t % 2
        device = peer(order[0], p1)
        if order[0] == "y":
            return remote(
                acc.at[w, t, :, pl.ds(pair_start(p1), 2), rows], r1y.at[w, t, :, :, rows], s1s, first_sem(c, w, t), device
            )
        if order[0] == "x":
            n = 0 if p1 == 1 else xt
            item = xt * 4 + zt * 2 + (n + m) % 2
            sem = first_sem(c, w, 2 * xt)
        else:
            n = m if p1 == 1 else (m + zt) % 2
            item = zt * 4 + xt * 2 + n
            sem = first_sem(c, w, xt + zt * (2 - xt))
        return remote(acc.at[w, t, n, :, rows], r1.at[w, item, :, rows], s1s, sem, device)

    def direct(c, w, t):
        index, _, _, _, rows = c
        for k in (2, 1, 3):
            src = acc.at[w, t, :, ORDER.index(k), rows]
            if k == 2:
                dst, send, sem = r2.at[w, t // 2, pl.ds(t % 2 * 2, 2), rows], s2s, s2r.at[w, index]
            else:
                dst, send, sem = r1y.at[w, t, :, k // 2, rows], s1s, first_sem(c, w, t)
            remote(src, dst, send, sem, peer("y", k)).start()

    def begin(w, t):
        ys, rest = colours(w)[0:2], colours(w)[2:6]
        for c in rest:
            send1(c, w, t).start()
        if w == 0:
            for c in ys:
                send1(c, w, t).start()
        else:

            @pl.when(t // 4 == 0)
            def _():
                for c in ys:
                    send1(c, w, t).start()

            @pl.when(t // 4 == 1)
            def _():
                for c in ys:
                    direct(c, w, t)

    def wait_for(ref, sem):
        remote(ref, ref, s1s, sem, other_core).wait_recv()

    def send2(c, w, t, n, item):
        index, order, _, p2, rows = c
        device = peer(order[0], p2)
        if order[0] == "y":
            return remote(
                acc.at[w, t, :, ORDER.index(p2), rows], r2.at[w, t // 2, pl.ds(t % 2 * 2, 2), rows], s2s, s2r.at[w, index], device
            )
        return remote(acc.at[w, t, n, :, rows], r2.at[w, item, :, rows], s2s, s2r.at[w, index], device)

    def multiply(t, w, rel):
        product = jnp.dot(ct[rel, w], abuf[t], preferred_element_type=F32)
        product = product.astype(jnp.bfloat16).astype(F32)
        for hrel in (0, 1):
            for n in (0, 1):
                for lrel in (0, 1):
                    place = (n * 2 + lrel) * 128
                    yield n, ORDER.index(2 * hrel + lrel), product[hrel * 128 : hrel * 128 + 128, place : place + 128]

    def a_wait(g):
        pltpu.make_async_copy(abuf.at[g], abuf.at[g], a_sem.at[g]).wait()

    def for_other(g):
        for n, target, block in multiply(g % 8, g // 8, 1):
            dsend[g % 4, n, target] = block

    def own(g):
        for n, target, block in multiply(g % 8, g // 8, 0):
            acc[g // 8, g % 8, n, target] = block + drecv[g % 4, n, target]

    def first(g):
        for wave in (0, 1):

            @pl.when(g // 8 == wave)
            def _(wave=wave):
                begin(wave, g % 8)

    def second(w, t, axes="yxz"):
        xt, zt, m = t // 4, t // 2 % 2, t % 2

        def onward(c, n, item):
            rows = c[4]
            acc[w, t, n, :, rows] = acc[w, t, n, :, rows] + r1[w, item, :, rows]
            send2(c, w, t, n, item).start()

        ys, xs, zs = colours(w)[0:2], colours(w)[2:4], colours(w)[4:6]
        if "y" in axes:
            for c in ys:
                _, _, p1, p2, rows = c
                on = ORDER.index(p2)
                send1(c, w, t).wait_recv()
                for n in (0, 1):
                    acc[w, t, n, on, rows] = acc[w, t, n, on, rows] + r1y[w, t, n, onward_item(p1), rows]
                send2(c, w, t, 0, 0).start()

        if "x" in axes:

            @pl.when(t == 4)
            def _():
                for c in xs:
                    wait_for(r1.at[w, pl.ds(0, 4), :, c[4]], first_sem(c, w, 0))

            @pl.when(xt == 1)
            def _():
                for c in xs:
                    n = 1 if c[2] == 1 else 0
                    onward(c, n, zt * 2 + (n + m) % 2)

        if "z" in axes:

            @pl.when((zt == 1) & (m == 0))
            def _():
                for c in zs:
                    wait_for(r1.at[w, pl.ds(0, 2), :, c[4]], first_sem(c, w, xt))

            @pl.when(zt == 1)
            def _():
                for c in zs:
                    n = 1 - m if c[2] == 1 else m
                    onward(c, n, xt * 2 + n)

    def stage1(w):
        for c in colours(w)[2:6]:
            index, order, p1, _, rows = c
            wait_for(r1.at[w, pl.ds(4, 4), :, rows], first_sem(c, w, 2))
            wait_for(r2.at[w, :, :, rows], s2r.at[w, index])
            for item in range(4):
                t, n = unit_at(1, item) if order[0] == "x" else unit_at(item, 1)
                total = acc[w, t, n, :, rows] + (r1[w, 4 + item, :, rows] + r2[w, item, :, rows])
                place = ORDER.index(UNIT_ORDER[item])
                if order[0] == "x":
                    b2[w, :, place, rows] = total
                else:
                    b2[w, place, :, rows] = total
            spread2(c, w)
        for c in colours(w)[0:2]:
            index, _, p1, _, rows = c
            if w == 1:
                for t in range(4, 8):
                    send1(c, w, t).wait_recv()
            wait_for(r2.at[w, :, :, rows], s2r.at[w, index])
            for sx in range(4):
                for sz in range(4):
                    t, n = unit_at(sx, sz)
                    total = acc[w, t, n, KEEP, rows] + (r1y[w, t, n, kept_item(p1), rows] + r2[w, t // 2, t % 2 * 2 + n, rows])
                    if w == 1 and t >= 4:
                        total = total + r1y[w, t, n, onward_item(p1), rows]
                    b2[w, ORDER.index(UNIT_ORDER[sz]), ORDER.index(UNIT_ORDER[sx]), rows] = total
            spread2(c, w)

    def spread2(c, w):
        index, order, _, _, rows = c
        for n in FAR_FIRST:
            k = ORDER[n]
            remote(b2.at[w, n, :, rows], r3.at[w, n, :, rows], s3s, s3r.at[w, index], peer(order[1], k)).start()

    def spread3(c, w):
        index, order, _, _, rows = c
        for n in FAR_FIRST:
            k = ORDER[n]
            remote(b2.at[w, KEEP, n, rows], r4.at[w, n, rows], s4s, s4r.at[w, index], peer(order[2], k)).start()

    def in_order(w):
        every = colours(w)
        return every[2:6] + every[0:2]

    def stage2(w):
        for c in in_order(w):
            index, rows = c[0], c[4]
            wait_for(r3.at[w, :, :, rows], s3r.at[w, index])
            b2[w, KEEP, :, rows] = (b2[w, KEEP, :, rows] + r3[w, 0, :, rows]) + (r3[w, 1, :, rows] + r3[w, 2, :, rows])
            spread3(c, w)

    def stage3(w):
        for c in in_order(w):
            index, rows = c[0], c[4]
            wait_for(r4.at[w, :, rows], s4r.at[w, index])
            b2[w, KEEP, KEEP, rows] = (b2[w, KEEP, KEEP, rows] + r4[w, 0, rows]) + (r4[w, 1, rows] + r4[w, 2, rows])

    def spread4(w, n):
        to_core, device = ((core, far), (1 - core, far_other), (1 - core, other_core))[n]
        return remote(
            fin.at[w, pl.ds(to_core * 64, 64)],
            obuf.at[core, :, pl.ds(pl.multiple_of(yhi * 256 + w * 128, 128), 128)],
            es_sem, er_sem.at[w, n], device,
        )

    def stage4(w):
        fin[w] = b2[w, KEEP, KEEP].T
        for n in range(3):
            spread4(w, n).start()
        obuf[core, :, pl.ds(pl.multiple_of(yhi * 256 + w * 128, 128), 128)] = fin[w, pl.ds(core * 64, 64)]

    with jax.named_scope("start"):
        a_wait(0)
        for_other(0)
        transpose(0, 0)
        pl.semaphore_wait(barrier, len(peers))
        d2d(0).start()
        a_wait(1)
        for_other(1)
        d2d(1).start()

    def step(g, carry):
        @pl.when(g < 8)
        def _():
            a_wait(g)

        @pl.when(g >= 4)
        def _():
            d2d(g).wait_send()

        with jax.named_scope("d2dwait"):
            d2d(g - LAG1).wait_recv()
        with jax.named_scope("dots"):
            for_other(g)
            own(g - LAG1)
        d2d(g).start()
        first(g - LAG1)

        @pl.when(g == 3)
        def _():
            c_wait(1)
            transpose(1, 1)
            transpose(0, 1)

        for wave in (0, 1):

            @pl.when((g >= LAG2 + 8 * wave) & (g < LAG2 + 8 * wave + 8))
            def _(wave=wave):
                with jax.named_scope("second"):
                    second(wave, g - LAG2 - 8 * wave)

        return carry

    lax.fori_loop(LAG1, 16, step, 0)

    for g in range(16, 16 + LAG1):
        with jax.named_scope("own"):
            d2d(g - LAG1).wait_recv()
            own(g - LAG1)
            begin(1, g - LAG1 - 8)
    left = range(8 - LAG2, 8)
    with jax.named_scope("second"):
        for t in left:
            second(1, t, "x")
        for t in left:
            second(1, t, "yz" if t < 4 else "z")

    for name, stage, w in (
        ("e1", stage1, 0), ("f1", stage1, 1), ("e2", stage2, 0), ("f2", stage2, 1), ("e3", stage3, 0), ("e4", stage4, 0),
        ("f3", stage3, 1), ("f4", stage4, 1),
    ):
        with jax.named_scope(name):
            stage(w)

    with jax.named_scope("swapwait"):
        for w in (0, 1):
            for n in range(3):
                spread4(w, n).wait_recv()
        out[...] = obuf[...]

    with jax.named_scope("ends"):
        for wave in (0, 1):
            rest = colours(wave)[2:6]
            for whole in (
                r1y.at[wave, :, :, :, pl.ds(0, SIZES[wave][0] + SIZES[wave][1])],
                r1.at[wave, :, :, pl.ds(rest[0][4].start, 128 - rest[0][4].start)],
            ):
                remote(whole, whole, s1s, er_sem.at[0, 0], other_core).wait_send()
        for whole, sem in (
            (r2, s2s), (r3, s3s), (r4, s4s), (r2.at[0, 0, pl.ds(0, 3)], es_sem)
        ):
            remote(whole, whole, sem, er_sem.at[0, 0], other_core).wait_send()
        for g in range(12, 16):
            d2d(g).wait_send()


def local(activations, key_cotangent, value_cotangent):
    tok, width = activations.shape
    half = key_cotangent.shape[1]
    rows = width // 64
    y_rows = max(sizes[0] + sizes[1] for sizes in SIZES)
    dma = pltpu.SemaphoreType.DMA
    both = pl.pallas_call(
        kernel,
        out_shape=jax.ShapeDtypeStruct((2, rows, half), F32),
        in_specs=[pl.BlockSpec(memory_space=pl.ANY)] * 3,
        out_specs=pl.BlockSpec(memory_space=pltpu.VMEM),
        scratch_shapes=[
            pltpu.VMEM((8, tok, 512), jnp.bfloat16),
            pltpu.VMEM((2, 2, 2, tok, 128), jnp.bfloat16),
            pltpu.VMEM((2, 2, 256, tok), jnp.bfloat16),
            pltpu.VMEM((2, 8, 2, 4, 128, 128), F32),
            pltpu.VMEM((4, 2, 4, 128, 128), F32),
            pltpu.VMEM((4, 2, 4, 128, 128), F32),
            pltpu.VMEM((2, 8, 4, 128, 128), F32),
            pltpu.VMEM((2, 8, 2, 2, y_rows, 128), F32),
            pltpu.VMEM((2, 4, 4, 128, 128), F32),
            pltpu.VMEM((2, 4, 4, 128, 128), F32),
            pltpu.VMEM((2, 3, 4, 128, 128), F32),
            pltpu.VMEM((2, 3, 128, 128), F32),
            pltpu.VMEM((2, 128, 128), F32),
            pltpu.VMEM((2, rows, half), F32),
            dma((8,)), dma((2,)), dma((4,)), dma((4,)),
            dma, dma((2, 28)), dma, dma((2, 6)),
            dma, dma((2, 6)), dma, dma((2, 6)),
            dma, dma((2, 3)),
        ],
        compiler_params=pltpu.CompilerParams(
            collective_id=0, has_side_effects=True, vmem_limit_bytes=LIMIT
        ),
        name="weight_gradients",
    )(activations, key_cotangent, value_cotangent)
    return both[0], both[1]


def solution(mesh):
    finer = Mesh(mesh.devices.reshape(mesh.shape["inter"], 4, 2, 4, 2), AXES)
    spec = P(AXES, None)
    out = P(INTRA, None)
    return jax.shard_map(local, mesh=finer, in_specs=(spec, spec, spec), out_specs=(out, out), check_vma=False)
```
